32 devices in a mesh: row: 4 (over y, x), col: 8 (over z, core).
Axes of the slice: x: 2, y: 2, z: 4, core: 2. Of those that a mesh axis runs over, the one named last changes fastest.
Arguments:
- left_matrix: float32 [4096, 4096], P('row', 'col'), may hold values from -6 to 6
- right_matrix: float32 [4096, 4096], P('row', 'col'), may hold values from -0.09375 to 0.09375
Outputs:
- product_matrix: float32 [4096, 4096], P('row', 'col')
The draws below stay inside these ranges and needn't reach their ends.
All inputs are finite; a program needn't handle non-finite values.
Results may differ from the reference program's by a relative error of at most 0.00019.
Values sent between devices are 32-bit elements; how exact they have to be, the bound alone decides.
A program may use at most 64 MiB of HBM per device.

```python
import jax
import jax.numpy as jnp
from jax import lax

ORDER = 4096


def level_of(own_key, dims, split, least, high):
    def one(position, blocks):
        steps = jax.random.uniform(jax.random.fold_in(jax.random.fold_in(own_key, 6), position), (blocks,), jnp.float32, least / len(split), high / len(split))
        return jnp.repeat(jnp.exp(steps), dims[position] // blocks).reshape((-1,) + (1,) * (len(dims) - position - 1))

    gain = one(*split[0])
    for cut in split[1:]:
        gain = gain * one(*cut)
    return gain


def scatter_about(own_key, extent, spread, reach, split=(), dtype=jnp.bfloat16):
    gain = level_of(own_key, extent, split, -0.22, 0.18) if split else 1.0
    result = jax.random.normal(own_key, extent, jnp.float32) * spread * gain
    return jnp.minimum(jnp.maximum(result, -reach), reach).astype(dtype)


def setup_inputs(seed: int = 0) -> dict:
    arg_keys = jax.random.split(jax.random.key(seed), 3)
    left_matrix = scatter_about(arg_keys[0], (ORDER, ORDER), 1.0, 6.0, ((0, 4), (1, 8)), jnp.float32)
    right_matrix = scatter_about(arg_keys[1], (ORDER, ORDER), ORDER ** -0.5, 0.09375, ((0, 4), (1, 8)), jnp.float32)
    return {"left_matrix": left_matrix, "right_matrix": right_matrix}


def multiply(left_term, right_term):
    return jnp.dot(left_term, right_term, precision=lax.Precision.HIGHEST, preferred_element_type=jnp.float32)


def left_terms(upper_left, upper_right, lower_left, lower_right):
    sum_one = lower_left + lower_right
    sum_two = sum_one - upper_left
    sum_three = upper_left - lower_left
    sum_four = upper_right - sum_two
    return (upper_left, upper_right, sum_four, lower_right, sum_one, sum_two, sum_three)


def right_terms(upper_left, upper_right, lower_left, lower_right):
    diff_one = upper_right - upper_left
    diff_two = lower_right - diff_one
    diff_three = lower_right - upper_right
    diff_four = diff_two - lower_left
    return (upper_left, lower_left, lower_right, diff_four, diff_one, diff_two, diff_three)


def reference(left_matrix, right_matrix):
    half_order = ORDER // 2
    lefts = left_terms(left_matrix[:half_order, :half_order], left_matrix[:half_order, half_order:],
                       left_matrix[half_order:, :half_order], left_matrix[half_order:, half_order:])
    rights = right_terms(right_matrix[:half_order, :half_order], right_matrix[:half_order, half_order:],
                         right_matrix[half_order:, :half_order], right_matrix[half_order:, half_order:])
    products = [multiply(lefts[index], rights[index]) for index in range(7)]
    partial_two = products[0] + products[5]
    partial_three = partial_two + products[6]
    partial_four = partial_two + products[4]
    upper_left = products[0] + products[1]
    upper_right = partial_four + products[2]
    lower_left = partial_three - products[3]
    lower_right = partial_three + products[4]
    return jnp.block([[upper_left, upper_right], [lower_left, lower_right]])
```

```python
import functools

import jax
import jax.numpy as jnp
from jax import lax
from jax.experimental import pallas as pl
from jax.experimental.pallas import tpu as pltpu
from jax.sharding import PartitionSpec as P

MESH = pl.DeviceIdType.MESH
CHUNKS = 4


def split(value):
    high = value.astype(jnp.bfloat16)
    low = (value - high.astype(jnp.float32)).astype(jnp.bfloat16)
    return high, low


def kernel(rows, cols, a_in, b_in, out, a_all, b_all, b_high, b_low,
           a_recv, a_send, b_recv, b_send, local):
    row = lax.axis_index("row")
    col = lax.axis_index("col")
    core = lax.rem(col, 2)
    chip = lax.div(col, 2)
    chips = cols // 2
    height, a_depth = a_in.shape
    b_depth = b_in.shape[0]
    per_b = b_depth // a_depth
    size = height // CHUNKS
    partner = chip * 2 + 1 - core

    def left_valid(distance):
        return chip >= distance

    def right_valid(distance):
        return chip + distance < chips

    def a_copy(kind, block, chunk, own):
        part = pl.ds(chunk * size, size)
        target = (col + 2, col - 2, partner)[kind]
        return pltpu.make_async_remote_copy(
            src_ref=a_in.at[part] if own else a_all.at[block, part],
            dst_ref=a_all.at[block, part],
            send_sem=a_send.at[kind, block, chunk],
            recv_sem=a_recv.at[block, chunk],
            device_id={"col": target}, device_id_type=MESH)

    def a_wait(block, chunk):
        a_copy(2, block, chunk, False).wait_recv()

    def b_copy(peer, source):
        return pltpu.make_async_remote_copy(
            src_ref=b_in, dst_ref=b_all.at[source],
            send_sem=b_send.at[peer], recv_sem=b_recv.at[source],
            device_id={"row": peer}, device_id_type=MESH)

    barrier = pltpu.get_barrier_semaphore()

    @pl.when(chip > 0)
    def _():
        pl.semaphore_signal(barrier, inc=1, device_id={"col": col - 2}, device_id_type=MESH)

    @pl.when(chip < chips - 1)
    def _():
        pl.semaphore_signal(barrier, inc=1, device_id={"col": col + 2}, device_id_type=MESH)

    pl.semaphore_signal(barrier, inc=1, device_id={"col": partner}, device_id_type=MESH)
    peers = [lax.rem(row + offset, rows) for offset in range(1, rows)]
    for peer in peers:
        pl.semaphore_signal(barrier, inc=1, device_id={"row": peer}, device_id_type=MESH)
    own_a = pltpu.make_async_copy(a_in, a_all.at[col], local.at[0])
    own_b = pltpu.make_async_copy(b_in, b_all.at[row], local.at[1])
    own_a.start()
    own_b.start()
    near = jnp.where(chip > 0, 1, 0) + jnp.where(chip < chips - 1, 1, 0)
    pl.semaphore_wait(barrier, rows + near)

    for chunk in range(CHUNKS):
        @pl.when(right_valid(1))
        def _():
            a_copy(0, col, chunk, True).start()

        @pl.when(left_valid(1))
        def _():
            a_copy(1, col, chunk, True).start()
    for peer in peers:
        b_copy(peer, row).start()
    for chunk in range(CHUNKS):
        a_copy(2, col, chunk, True).start()

    out[...] = jnp.zeros_like(out)
    own_a.wait()
    own_b.wait()

    def multiply(block, chunk):
        part = pl.ds(pl.multiple_of(chunk * size, size), size)
        source = lax.div(block, per_b)
        offset = pl.multiple_of(lax.rem(block, per_b) * a_depth, a_depth)
        depth = pl.ds(offset, a_depth)
        high, low = split(a_all[block, part, :])
        right_high = b_high[source, depth, :]
        right_low = b_low[source, depth, :]
        dot = functools.partial(jnp.dot, preferred_element_type=jnp.float32)
        out[part, :] += (dot(low, right_high) + dot(high, right_low)) + dot(high, right_high)

    def split_b(source):
        @pl.loop(0, b_depth // 128)
        def _(index):
            part = pl.ds(pl.multiple_of(index * 128, 128), 128)
            high, low = split(b_all[source, part, :])
            b_high[source, part, :] = high
            b_low[source, part, :] = low

    def multiply_block(block):
        @pl.loop(0, CHUNKS)
        def _(chunk):
            multiply(block, chunk)

    for distance in range(1, chips - 1):
        for chunk in range(CHUNKS):
            @pl.when(left_valid(distance))
            def _():
                block = col - 2 * distance
                a_wait(block, chunk)

                @pl.when(right_valid(1))
                def _():
                    a_copy(0, block, chunk, False).start()
                a_copy(2, block, chunk, False).start()

            @pl.when(right_valid(distance))
            def _():
                block = col + 2 * distance
                a_wait(block, chunk)

                @pl.when(left_valid(1))
                def _():
                    a_copy(1, block, chunk, False).start()
                a_copy(2, block, chunk, False).start()

    split_b(row)
    for peer in peers:
        b_copy(peer, peer).wait_recv()
        split_b(peer)

    for chunk in range(CHUNKS):
        a_wait(partner, chunk)
    multiply_block(col)
    multiply_block(partner)
    for distance in range(1, chips - 1):
        for valid, step in ((left_valid, -2), (right_valid, 2)):
            @pl.when(valid(distance))
            def _():
                for chunk in range(CHUNKS):
                    a_wait(partner + step * distance, chunk)
                multiply_block(col + step * distance)
                multiply_block(partner + step * distance)

    if chips > 1:
        for valid, step in ((left_valid, -2), (right_valid, 2)):
            @pl.when(valid(chips - 1))
            def _():
                block = col + step * (chips - 1)
                other = partner + step * (chips - 1)
                for chunk in range(CHUNKS):
                    a_wait(block, chunk)
                    a_copy(2, block, chunk, False).start()
                    multiply(block, chunk)
                    a_wait(other, chunk)
                    multiply(other, chunk)

    for peer in peers:
        b_copy(peer, row).wait_send()
    for chunk in range(CHUNKS):
        a_copy(2, col, chunk, True).wait_send()
        for distance in range(0, chips):
            @pl.when(left_valid(distance) & right_valid(1))
            def _():
                a_copy(0, col - 2 * distance, chunk, False).wait_send()

            @pl.when(right_valid(distance) & left_valid(1))
            def _():
                a_copy(1, col + 2 * distance, chunk, False).wait_send()
        for distance in range(1, chips):
            @pl.when(left_valid(distance))
            def _():
                a_copy(2, col - 2 * distance, chunk, False).wait_send()

            @pl.when(right_valid(distance))
            def _():
                a_copy(2, col + 2 * distance, chunk, False).wait_send()


def body(rows, cols, left_matrix, right_matrix):
    height, a_depth = left_matrix.shape
    b_depth, width = right_matrix.shape
    return pl.pallas_call(
        functools.partial(kernel, rows, cols),
        out_shape=jax.ShapeDtypeStruct((height, width), jnp.float32),
        in_specs=[pl.BlockSpec(memory_space=pl.ANY)] * 2,
        out_specs=pl.BlockSpec(memory_space=pltpu.VMEM),
        scratch_shapes=[
            pltpu.VMEM((cols, height, a_depth), jnp.float32),
            pltpu.VMEM((rows, b_depth, width), jnp.float32),
            pltpu.VMEM((rows, b_depth, width), jnp.bfloat16),
            pltpu.VMEM((rows, b_depth, width), jnp.bfloat16),
            pltpu.SemaphoreType.DMA((cols, CHUNKS)),
            pltpu.SemaphoreType.DMA((3, cols, CHUNKS)),
            pltpu.SemaphoreType.DMA((rows,)),
            pltpu.SemaphoreType.DMA((rows,)),
            pltpu.SemaphoreType.DMA((2,)),
        ],
        compiler_params=pltpu.CompilerParams(
            collective_id=0, has_side_effects=True, vmem_limit_bytes=56 * 2**20),
    )(left_matrix, right_matrix)


def solution(mesh):
    placed = (P("row", "col"), P("row", "col"))
    return jax.shard_map(
        functools.partial(body, mesh.shape["row"], mesh.shape["col"]),
        mesh=mesh, in_specs=placed, out_specs=P("row", "col"), check_vma=False
    )
```

```python
import functools

import jax
import jax.numpy as jnp
from jax import lax
from jax.experimental import pallas as pl
from jax.experimental.pallas import tpu as pltpu
from jax.sharding import PartitionSpec as P

MESH = pl.DeviceIdType.MESH
CHUNKS = 4


def split(value):
    high = value.astype(jnp.bfloat16)
    low = (value - high.astype(jnp.float32)).astype(jnp.bfloat16)
    return high, low


def kernel(rows, cols, a_in, b_in, out, a_all, b_all, b_high, b_low,
           a_recv, a_send, b_recv, b_send, local):
    row = lax.axis_index("row")
    col = lax.axis_index("col")
    core = lax.rem(col, 2)
    chip = lax.div(col, 2)
    chips = cols // 2
    height, a_depth = a_in.shape
    b_depth = b_in.shape[0]
    per_b = b_depth // a_depth
    size = height // CHUNKS
    partner = chip * 2 + 1 - core

    def left_valid(distance):
        return chip >= distance

    def right_valid(distance):
        return chip + distance < chips

    def a_copy(kind, block, chunk, own):
        part = pl.ds(chunk * size, size)
        target = (col + 2, col - 2, partner)[kind]
        return pltpu.make_async_remote_copy(
            src_ref=a_in.at[part] if own else a_all.at[block, part],
            dst_ref=a_all.at[block, part],
            send_sem=a_send.at[kind, block, chunk],
            recv_sem=a_recv.at[block, chunk],
            device_id={"col": target}, device_id_type=MESH)

    def a_wait(block, chunk):
        a_copy(2, block, chunk, False).wait_recv()

    def b_copy(peer, source):
        return pltpu.make_async_remote_copy(
            src_ref=b_in, dst_ref=b_all.at[source],
            send_sem=b_send.at[peer], recv_sem=b_recv.at[source],
            device_id={"row": peer}, device_id_type=MESH)

    barrier = pltpu.get_barrier_semaphore()

    @pl.when(chip > 0)
    def _():
        pl.semaphore_signal(barrier, inc=1, device_id={"col": col - 2}, device_id_type=MESH)

    @pl.when(chip < chips - 1)
    def _():
        pl.semaphore_signal(barrier, inc=1, device_id={"col": col + 2}, device_id_type=MESH)

    pl.semaphore_signal(barrier, inc=1, device_id={"col": partner}, device_id_type=MESH)
    peers = [lax.rem(row + offset, rows) for offset in range(1, rows)]
    for peer in peers:
        pl.semaphore_signal(barrier, inc=1, device_id={"row": peer}, device_id_type=MESH)
    own_a = pltpu.make_async_copy(a_in, a_all.at[col], local.at[0])
    own_b = pltpu.make_async_copy(b_in, b_all.at[row], local.at[1])
    own_a.start()
    own_b.start()
    near = jnp.where(chip > 0, 1, 0) + jnp.where(chip < chips - 1, 1, 0)
    pl.semaphore_wait(barrier, rows + near)

    for chunk in range(CHUNKS):
        @pl.when(right_valid(1))
        def _():
            a_copy(0, col, chunk, True).start()

        @pl.when(left_valid(1))
        def _():
            a_copy(1, col, chunk, True).start()
    for peer in peers:
        b_copy(peer, row).start()
    for chunk in range(CHUNKS):
        a_copy(2, col, chunk, True).start()

    out[...] = jnp.zeros_like(out)
    own_a.wait()
    own_b.wait()

    def multiply(block, chunk):
        part = pl.ds(pl.multiple_of(chunk * size, size), size)
        source = lax.div(block, per_b)
        offset = pl.multiple_of(lax.rem(block, per_b) * a_depth, a_depth)
        depth = pl.ds(offset, a_depth)
        high, low = split(a_all[block, part, :])
        right_high = b_high[source, depth, :]
        right_low = b_low[source, depth, :]
        dot = functools.partial(jnp.dot, preferred_element_type=jnp.float32)
        out[part, :] += (dot(low, right_high) + dot(high, right_low)) + dot(high, right_high)

    def split_b(source):
        @pl.loop(0, b_depth // 128)
        def _(index):
            part = pl.ds(pl.multiple_of(index * 128, 128), 128)
            high, low = split(b_all[source, part, :])
            b_high[source, part, :] = high
            b_low[source, part, :] = low

    def multiply_block(block):
        @pl.loop(0, CHUNKS)
        def _(chunk):
            multiply(block, chunk)

    for distance in range(1, chips - 1):
        for chunk in range(CHUNKS):
            @pl.when(left_valid(distance))
            def _():
                block = col - 2 * distance
                a_wait(block, chunk)

                @pl.when(right_valid(1))
                def _():
                    a_copy(0, block, chunk, False).start()
                a_copy(2, block, chunk, False).start()

            @pl.when(right_valid(distance))
            def _():
                block = col + 2 * distance
                a_wait(block, chunk)

                @pl.when(left_valid(1))
                def _():
                    a_copy(1, block, chunk, False).start()
                a_copy(2, block, chunk, False).start()

    split_b(row)
    for peer in peers:
        b_copy(peer, peer).wait_recv()
        split_b(peer)

    for chunk in range(CHUNKS):
        a_wait(partner, chunk)
    multiply_block(col)
    multiply_block(partner)
    for distance in range(1, chips - 1):
        for valid, step in ((left_valid, -2), (right_valid, 2)):
            @pl.when(valid(distance))
            def _():
                for chunk in range(CHUNKS):
                    a_wait(partner + step * distance, chunk)
                multiply_block(col + step * distance)
                multiply_block(partner + step * distance)

    if chips > 1:
        for valid, step in ((left_valid, -2), (right_valid, 2)):
            @pl.when(valid(chips - 1))
            def _():
                block = col + step * (chips - 1)
                other = partner + step * (chips - 1)
                for chunk in range(CHUNKS):
                    a_wait(block, chunk)
                    a_copy(2, block, chunk, False).start()
                    multiply(block, chunk)
                    a_wait(other, chunk)
                    multiply(other, chunk)

    for peer in peers:
        b_copy(peer, row).wait_send()
    for chunk in range(CHUNKS):
        a_copy(2, col, chunk, True).wait_send()
        for distance in range(0, chips):
            @pl.when(left_valid(distance) & right_valid(1))
            def _():
                a_copy(0, col - 2 * distance, chunk, False).wait_send()

            @pl.when(right_valid(distance) & left_valid(1))
            def _():
                a_copy(1, col + 2 * distance, chunk, False).wait_send()
        for distance in range(1, chips):
            @pl.when(left_valid(distance))
            def _():
                a_copy(2, col - 2 * distance, chunk, False).wait_send()

            @pl.when(right_valid(distance))
            def _():
                a_copy(2, col + 2 * distance, chunk, False).wait_send()


def body(rows, cols, left_matrix, right_matrix):
    height, a_depth = left_matrix.shape
    b_depth, width = right_matrix.shape
    return pl.pallas_call(
        functools.partial(kernel, rows, cols),
        out_shape=jax.ShapeDtypeStruct((height, width), jnp.float32),
        in_specs=[pl.BlockSpec(memory_space=pl.ANY)] * 2,
        out_specs=pl.BlockSpec(memory_space=pltpu.VMEM),
        scratch_shapes=[
            pltpu.VMEM((cols, height, a_depth), jnp.float32),
            pltpu.VMEM((rows, b_depth, width), jnp.float32),
            pltpu.VMEM((rows, b_depth, width), jnp.bfloat16),
            pltpu.VMEM((rows, b_depth, width), jnp.bfloat16),
            pltpu.SemaphoreType.DMA((cols, CHUNKS)),
            pltpu.SemaphoreType.DMA((3, cols, CHUNKS)),
            pltpu.SemaphoreType.DMA((rows,)),
            pltpu.SemaphoreType.DMA((rows,)),
            pltpu.SemaphoreType.DMA((2,)),
        ],
        compiler_params=pltpu.CompilerParams(
            collective_id=0, has_side_effects=True, vmem_limit_bytes=56 * 2**20),
    )(left_matrix, right_matrix)


STEPS = 8
LAG = 2
EARLY = 2


def shared_kernel(a_in, b_in, out, a_all, b_all, b_high, b_low, c_all, c_high, c_low, partial,
                  a_recv, a_send, b_recv, b_send, c_recv, c_send, p_recv, p_send, local):
    row = lax.axis_index("row")
    col = lax.axis_index("col")
    core = lax.rem(col, 2)
    chip = lax.div(col, 2)
    partner = chip * 2 + 1 - core
    side = lax.div(chip, 2)
    y = lax.div(row, 2)
    x = lax.rem(row, 2)
    x_near = y * 2 + 1 - x
    y_near = (1 - y) * 2 + x
    far_corner = (1 - y) * 2 + 1 - x
    other_side = 1 - side
    end = 6 * side + core
    middle = 2 + 2 * side + core
    other_middle = 4 - 2 * side + core
    other_end = 6 - 6 * side + core
    swap = 1 - 2 * core
    is_end = (chip == 0) | (chip == 3)
    is_middle = (chip == 1) | (chip == 2)
    height, a_depth = a_in.shape
    b_depth = b_in.shape[0]
    a_size = height // STEPS
    b_size = b_depth // STEPS

    def a_copy(kind, target, block, step, own=False):
        part = pl.ds(step * a_size, a_size)
        return pltpu.make_async_remote_copy(
            src_ref=a_in.at[part] if own else a_all.at[block, part],
            dst_ref=a_all.at[block, part],
            send_sem=a_send.at[kind, block, step], recv_sem=a_recv.at[block, step],
            device_id={"col": target}, device_id_type=MESH)

    def a_wait(block, step):
        a_copy(2, partner, block, step).wait_recv()

    def b_copy(kind, target, source, step, own=False):
        part = pl.ds(step * b_size, b_size)
        return pltpu.make_async_remote_copy(
            src_ref=b_in.at[part] if own else b_all.at[source, part],
            dst_ref=b_all.at[source, part],
            send_sem=b_send.at[kind, step], recv_sem=b_recv.at[source, step],
            device_id={"row": target}, device_id_type=MESH)

    def b_wait(source):
        for step in range(STEPS):
            b_copy(0, x_near, source, step).wait_recv()

    def c_down(step, own):
        part = pl.ds(step * b_size, b_size)
        return pltpu.make_async_remote_copy(
            src_ref=b_in.at[part] if own else b_all.at[y_near, part],
            dst_ref=c_all.at[x, part],
            send_sem=c_send.at[0, step], recv_sem=c_recv.at[x, step],
            device_id={"col": middle}, device_id_type=MESH)

    def c_across(slot, step):
        part = pl.ds(step * b_size, b_size)
        return pltpu.make_async_remote_copy(
            src_ref=c_all.at[slot, part], dst_ref=c_all.at[slot, part],
            send_sem=c_send.at[1, step], recv_sem=c_recv.at[slot, step],
            device_id={"row": x_near}, device_id_type=MESH)

    def p_copy(step):
        part = pl.ds(step * a_size, a_size)
        return pltpu.make_async_remote_copy(
            src_ref=partial.at[part], dst_ref=partial.at[part],
            send_sem=p_send.at[step], recv_sem=p_recv.at[step],
            device_id={"col": end}, device_id_type=MESH)

    def split_into(source, full, high_all, low_all):
        @pl.loop(0, b_depth // 128)
        def _(index):
            part = pl.ds(pl.multiple_of(index * 128, 128), 128)
            high, low = split(full[source, part, :])
            high_all[source, part, :] = high
            low_all[source, part, :] = low

    dot = functools.partial(jnp.dot, preferred_element_type=jnp.float32)

    def multiply(into, part, block, high_all, low_all, source, half):
        depth = pl.ds(pl.multiple_of(half * a_depth, a_depth), a_depth)
        high, low = split(a_all[block, part, :])
        right_high = high_all[source, depth, :]
        right_low = low_all[source, depth, :]
        into[part, :] += (dot(low, right_high) + dot(high, right_low)) + dot(high, right_high)

    def multiply_source(source):
        @pl.loop(0, 8)
        def _(index):
            size = height // 4
            part = pl.ds(pl.multiple_of(lax.rem(index, 4) * size, size), size)
            half = lax.div(index, 4)
            multiply(out, part, 2 * source + half, b_high, b_low, source, half)

    barrier = pltpu.get_barrier_semaphore()

    def greet(target):
        pl.semaphore_signal(barrier, inc=1, device_id=target, device_id_type=MESH)

    greet({"col": partner})
    for peer in (x_near, y_near, far_corner):
        greet({"row": peer})

    @pl.when(is_end)
    def _():
        greet({"col": middle})

    @pl.when(is_middle)
    def _():
        greet({"col": end})
        greet({"col": other_middle})

    own_a = pltpu.make_async_copy(a_in, a_all.at[col], local.at[0])
    own_b = pltpu.make_async_copy(b_in, b_all.at[row], local.at[1])
    own_a.start()
    own_b.start()
    pl.semaphore_wait(barrier, jnp.where(is_end, 5, 6))

    @pl.when(is_end)
    def _():
        donor = y == other_side
        keeper = y == side

        @pl.when(donor)
        def _():
            for step in range(STEPS):
                c_down(step, True).start()
                b_copy(1, y_near, row, step, True).start()

        @pl.when(keeper)
        def _():
            for step in range(STEPS):
                b_copy(0, x_near, row, step, True).start()
                b_copy(1, y_near, row, step, True).start()
            for step in range(STEPS):
                b_copy(2, far_corner, row, step, True).start()

        for step in range(STEPS):
            a_copy(2, partner, col, step, True).start()
        out[...] = jnp.zeros_like(out)
        own_a.wait()
        own_b.wait()

        @pl.when(keeper)
        def _():
            for step in range(STEPS):
                b_copy(1, y_near, y_near, step).wait_recv()
                c_down(step, False).start()

        for step in range(STEPS):
            a_copy(0, middle, col, step, True).start()
        for step in range(STEPS):
            a_wait(middle, step)
            a_copy(2, partner, middle, step).start()

        @pl.when(donor)
        def _():
            b_wait(y_near)
            b_wait(far_corner)

        @pl.when(keeper)
        def _():
            b_wait(x_near)

        for step in range(STEPS):
            a_wait(end + swap, step)
            a_wait(middle + swap, step)
        for index in range(2):
            split_into(2 * side + index, b_all, b_high, b_low)
            multiply_source(2 * side + index)
        for step in range(STEPS):
            part = pl.ds(step * a_size, a_size)
            p_copy(step).wait_recv()
            out[part, :] += partial[part, :]

        @pl.when(donor)
        def _():
            for step in range(STEPS):
                c_down(step, True).wait_send()
                b_copy(1, y_near, row, step, True).wait_send()

        @pl.when(keeper)
        def _():
            for step in range(STEPS):
                for kind, peer in enumerate((x_near, y_near, far_corner)):
                    b_copy(kind, peer, row, step, True).wait_send()
                c_down(step, False).wait_send()
        for step in range(STEPS):
            a_copy(2, partner, col, step, True).wait_send()
            a_copy(0, middle, col, step, True).wait_send()
            a_copy(2, partner, middle, step).wait_send()

    @pl.when(is_middle)
    def _():
        sent = []

        def go(copy):
            copy.start()
            sent.append(copy)

        for step in range(STEPS):
            go(a_copy(1, end, col, step, True))
            go(a_copy(0, other_middle, col, step, True))
        for step in range(EARLY):
            go(b_copy(0, x_near, row, step, True))
        for step in range(STEPS):
            go(b_copy(1, y_near, row, step, True))
        for step in range(STEPS):
            go(a_copy(2, partner, col, step, True))
        out[...] = jnp.zeros_like(out)
        partial[...] = jnp.zeros_like(partial)
        own_a.wait()
        own_b.wait()
        split_into(row, b_all, b_high, b_low)

        for step in range(STEPS):
            c_across(x, step).wait_recv()
            go(c_across(x, step))
            a_wait(other_middle, step)
            go(a_copy(2, partner, other_middle, step))
        for step in range(EARLY, STEPS):
            go(b_copy(0, x_near, row, step, True))
        split_into(x, c_all, c_high, c_low)

        for step in range(STEPS + LAG):
            if step < STEPS:
                a_wait(end, step)
                go(a_copy(0, other_middle, end, step))
                go(a_copy(2, partner, end, step))
            if step < LAG:
                continue
            if step == LAG:
                b_wait(y_near)
                split_into(y_near, b_all, b_high, b_low)
                for index in range(STEPS):
                    c_across(1 - x, index).wait_recv()
                split_into(1 - x, c_all, c_high, c_low)
            late = step - LAG
            part = pl.ds(late * a_size, a_size)
            a_wait(other_end, late)
            go(a_copy(2, partner, other_end, late))
            for block in (middle, other_middle, end, other_end):
                a_wait(block + swap, late)

            @pl.loop(0, 4)
            def _(index):
                multiply(partial, part, 4 * other_side + index, c_high, c_low,
                         lax.div(index, 2), lax.rem(index, 2))

            @pl.loop(0, 4)
            def _(index):
                source = lax.div(index, 2) * 2 + x
                half = lax.rem(index, 2)
                multiply(out, part, 2 * source + half, b_high, b_low, source, half)

            go(p_copy(late))
            b_copy(0, x_near, x_near, late).wait_recv()
            go(b_copy(2, y_near, x_near, late))

        split_into(x_near, b_all, b_high, b_low)
        multiply_source(x_near)
        b_wait(far_corner)
        split_into(far_corner, b_all, b_high, b_low)
        multiply_source(far_corner)
        for copy in sent:
            copy.wait_send()


def shared_body(left_matrix, right_matrix):
    height, a_depth = left_matrix.shape
    b_depth, width = right_matrix.shape
    dma = pltpu.SemaphoreType.DMA
    return pl.pallas_call(
        shared_kernel,
        out_shape=jax.ShapeDtypeStruct((height, width), jnp.float32),
        in_specs=[pl.BlockSpec(memory_space=pl.ANY)] * 2,
        out_specs=pl.BlockSpec(memory_space=pltpu.VMEM),
        scratch_shapes=[
            pltpu.VMEM((8, height, a_depth), jnp.float32),
            pltpu.VMEM((4, b_depth, width), jnp.float32),
            pltpu.VMEM((4, b_depth, width), jnp.bfloat16),
            pltpu.VMEM((4, b_depth, width), jnp.bfloat16),
            pltpu.VMEM((2, b_depth, width), jnp.float32),
            pltpu.VMEM((2, b_depth, width), jnp.bfloat16),
            pltpu.VMEM((2, b_depth, width), jnp.bfloat16),
            pltpu.VMEM((height, width), jnp.float32),
            dma((8, STEPS)), dma((3, 8, STEPS)), dma((4, STEPS)), dma((3, STEPS)),
            dma((2, STEPS)), dma((2, STEPS)), dma((STEPS,)), dma((STEPS,)), dma((2,)),
        ],
        compiler_params=pltpu.CompilerParams(
            collective_id=1, has_side_effects=True, vmem_limit_bytes=60 * 2**20),
    )(left_matrix, right_matrix)


def solution(mesh):
    placed = (P("row", "col"), P("row", "col"))
    rows, cols = mesh.shape["row"], mesh.shape["col"]
    part = shared_body if (rows, cols) == (4, 8) else functools.partial(body, rows, cols)
    return jax.shard_map(
        part, mesh=mesh, in_specs=placed, out_specs=P("row", "col"), check_vma=False
    )
```
